32 devices in a mesh: groups: 2 (over y), res: 8 (over z, x), seq: 2 (over core).
Axes of the slice: x: 2, y: 2, z: 4, core: 2. Of those that a mesh axis runs over, the one named last changes fastest.
Arguments:
- alignment: bfloat16 [128, 32, 256], P(('groups', 'seq'), 'res'), parts along dimension 0, may hold values from -6 to 6
- ln_gain: float32 [256], replicated, may hold values from 0.1 to 1.9
- proj_left: bfloat16 [256, 32], replicated, may hold values from -0.375 to 0.375
- proj_right: bfloat16 [256, 32], replicated, may hold values from -0.375 to 0.375
- out_weight: bfloat16 [1024, 128], replicated, may hold values from -4 to 4
- out_bias: float32 [128], replicated, may hold values from -3 to 3
Outputs:
- pair_update: bfloat16 [64, 32, 128], P(('groups', 'res'), 'seq'), parts along dimension 0
The draws below stay inside these ranges and needn't reach their ends.
There are 2 independent parts, one for each index of `groups`. The reference program is written for one: setup_inputs(seed, part) draws one part's arguments, and reference() takes and returns one part's arrays. A program takes and returns all parts, laid end to end along the dimension named above; an argument that names none is the same for every part. Nothing has to cross between parts.
All inputs are finite; a program needn't handle non-finite values.
Results may differ from the reference program's by a relative error of at most 0.0095.
Values may be sent and summed in bfloat16 or wider, within the bound.
No kernel may reach another device: no remote copies, remote signals or barrier semaphores. Data moves between devices by JAX's collectives and lax.ppermute only.
A program may use at most 64 MiB of HBM per device.

```python
import math
import jax
import jax.numpy as jnp
from jax import lax

CM = 256
CH = 32
CZ = 128
SEQS = 64
RES = 32


def steps_of(rng, dims, cuts, smallest, largest):
    loudness, own = 1.0, jax.random.fold_in(rng, 6)
    for axis_at, blocks in cuts:
        draws = jnp.exp(jax.random.uniform(jax.random.fold_in(own, axis_at), (blocks,), jnp.float32, smallest / len(cuts), largest / len(cuts)))
        loudness = loudness * jnp.repeat(draws, dims[axis_at] // blocks).reshape([-1 if axis == axis_at else 1 for axis in range(len(dims))])
    return loudness


def normal_values(key, shape, width, most, shards=(), kind=jnp.bfloat16):
    values = width * jax.random.normal(key, shape, jnp.float32)
    if shards:
        values = values * steps_of(key, shape, shards, -0.22, 0.18)
    return jnp.clip(values, -most, most).astype(kind)


def setup_inputs(seed: int = 0, part: int = 0) -> dict:
    splits = jax.random.split(jax.random.key(seed), 7)
    part_keys = jax.random.split(jax.random.fold_in(splits[6], part), 7)
    return {
        "alignment": normal_values(part_keys[0], (SEQS, RES, CM), 1.0, 6.0, ((0, 2), (1, 8))),
        "ln_gain": jnp.clip(1.0 + 0.18 * jax.random.normal(splits[1], (CM,), jnp.float32), 0.1, 1.9),
        "proj_left": normal_values(splits[2], (CM, CH), CM ** -0.5, 0.375),
        "proj_right": normal_values(splits[3], (CM, CH), CM ** -0.5, 0.375),
        "out_weight": normal_values(splits[4], (CH * CH, CZ), (SEQS ** 0.5 / CH), 4.0),
        "out_bias": normal_values(splits[5], (CZ,), 0.5, 3.0, (), jnp.float32),
    }


def normalize(alignment, ln_gain):
    values = alignment.astype(jnp.float32)
    centred = values - lax.optimization_barrier(jnp.mean(values, axis=-1, keepdims=True))
    variance = lax.optimization_barrier(jnp.mean(centred * centred, axis=-1, keepdims=True))
    return (centred * lax.rsqrt(variance + 1e-05) * ln_gain).astype(jnp.bfloat16)

def project_in(normed, weight):
    flat_rows = normed.reshape(-1, normed.shape[2])
    projected = jnp.dot(flat_rows, weight, preferred_element_type=jnp.float32).astype(jnp.bfloat16)
    return projected.reshape(normed.shape[0], normed.shape[1], weight.shape[1])

def reference(alignment, ln_gain, proj_left, proj_right, out_weight, out_bias):
    normed = normalize(alignment, ln_gain)
    left_side = project_in(normed, proj_left)
    right_side = project_in(normed, proj_right)
    right_flat = right_side.reshape(SEQS, RES * CH)
    weight_full = out_weight.astype(jnp.float32)
    block_width = math.gcd(RES, 8)

    def row_block(position):
        picked = lax.dynamic_slice_in_dim(left_side, position * block_width, block_width, 1)
        picked = picked.reshape(SEQS, block_width * CH)
        outer_terms = lax.dot_general(picked, right_flat, (((0,), (0,)), ((), ())), preferred_element_type=jnp.float32) * (1.0 / SEQS)
        outer_terms = outer_terms.reshape(block_width, CH, RES, CH).transpose(0, 2, 1, 3).reshape(block_width * RES, CH * CH)
        projected = jnp.dot(outer_terms, weight_full, precision=lax.Precision.HIGHEST) + out_bias
        return projected.reshape(block_width, RES, CZ).astype(jnp.bfloat16)
    blocks = lax.map(row_block, jnp.arange(RES // block_width, dtype=jnp.int32))
    return blocks.reshape(RES, RES, CZ)
```

```python
import functools
import math

import jax
import jax.numpy as jnp
from jax import lax
from jax.experimental import pallas as pl
from jax.experimental.pallas import tpu as pltpu
from jax.sharding import PartitionSpec as P

def normalize(alignment, ln_gain):
    values = alignment.astype(jnp.float32)
    centred = values - jnp.mean(values, axis=-1, keepdims=True)
    variance = jnp.mean(centred * centred, axis=-1, keepdims=True)
    return (centred * lax.rsqrt(variance + 1e-05) * ln_gain).astype(jnp.bfloat16)


def pair_block(left_flat, columns, weight_full, inv_count):
    channels = columns.shape[2]
    col_count = columns.shape[1]
    row_count = left_flat.shape[1] // channels
    block_width = math.gcd(col_count, 64)

    def advance(position, totals):
        column_block = lax.dynamic_slice_in_dim(columns, position * block_width, block_width, 1)
        right_flat = column_block.reshape(columns.shape[0], block_width * channels)
        outer_terms = (
            lax.dot_general(
                left_flat, right_flat, (((0,), (0,)), ((), ())), preferred_element_type=jnp.float32
            )
            * inv_count
        )
        outer_terms = outer_terms.reshape(row_count, channels, block_width, channels).transpose(
            0, 2, 1, 3
        )
        outer_terms = outer_terms.reshape(row_count * block_width, channels * channels)
        projected = jnp.dot(outer_terms, weight_full, precision=lax.Precision.HIGHEST)
        projected = projected.reshape(row_count, block_width, weight_full.shape[1])
        return lax.dynamic_update_slice_in_dim(totals, projected, position * block_width, 1)

    totals = jnp.zeros((row_count, col_count, weight_full.shape[1]), jnp.float32)
    return lax.fori_loop(0, col_count // block_width, advance, totals)


def gathered(alignment, ln_gain, proj_left, proj_right, out_weight, out_bias):
    seq_shards = lax.axis_size("seq")
    local_seqs = alignment.shape[0]
    local_res = alignment.shape[1]
    channels = proj_left.shape[1]
    inv_count = 1.0 / (local_seqs * seq_shards)
    normed = normalize(alignment, ln_gain)
    flat_rows = normed.reshape(-1, normed.shape[2])
    both_sides = jnp.dot(
        flat_rows, jnp.concatenate((proj_left, proj_right), 1), preferred_element_type=jnp.float32
    )
    both_sides = both_sides.astype(jnp.bfloat16).reshape(local_seqs, local_res, 2 * channels)
    left_side = both_sides[:, :, :channels]
    right_side = both_sides[:, :, channels:]
    weight_full = out_weight.astype(jnp.float32)
    left_all = lax.all_gather(left_side, "seq", axis=0, tiled=True)
    left_flat = left_all.reshape(left_all.shape[0], local_res * channels)
    right_all = lax.all_gather(right_side, "res", axis=1, tiled=True)
    split_right = right_all.reshape(
        local_seqs, seq_shards, right_all.shape[1] // seq_shards, channels
    )
    arrived = lax.all_to_all(split_right, "seq", split_axis=1, concat_axis=0, tiled=True)
    squeezed = arrived.reshape(arrived.shape[0], arrived.shape[2], arrived.shape[3])
    summed = pair_block(left_flat, squeezed, weight_full, inv_count)
    return (summed + out_bias).astype(jnp.bfloat16)


VMEM = pl.BlockSpec(memory_space=pltpu.VMEM)


def project_kernel(x_ref, gain_ref, left_ref, right_ref, both_ref):
    seqs = both_ref.shape[1]
    width = gain_ref.shape[1]
    local_res = x_ref.shape[1] // width
    sides = ([], [])
    for r in range(local_res):
        values = x_ref[:, r * width : (r + 1) * width].astype(jnp.float32)
        centred = values - jnp.mean(values, axis=-1, keepdims=True)
        variance = jnp.mean(centred * centred, axis=-1, keepdims=True)
        normed = (centred * lax.rsqrt(variance + 1e-05) * gain_ref[...]).astype(jnp.bfloat16)
        for side, weight_ref in zip(sides, (left_ref, right_ref)):
            side.append(
                lax.dot_general(
                    normed, weight_ref[...], (((1,), (1,)), ((), ())),
                    preferred_element_type=jnp.float32,
                )
            )
    for n, side in enumerate(sides):
        both_ref[n] = jnp.concatenate(side, axis=1).astype(jnp.bfloat16)


def pair_kernel(pitch, place_ref, left_ref, *refs):
    *right_refs, weight_ref, bias_ref, out_ref, terms, rows = refs
    pieces = len(right_refs)
    local_res, _, features = out_ref.shape
    lanes = left_ref.shape[1]
    channels = lanes // local_res
    per_piece = lanes // channels
    inv_count = 1.0 / left_ref.shape[0]
    left_t = left_ref[...].T
    for n, right_ref in enumerate(right_refs):
        product = jnp.dot(left_t, right_ref[...], preferred_element_type=jnp.float32)
        at = place_ref[0] ^ n
        for i in range(local_res):
            first = pl.multiple_of((i * pieces + at) * pitch, 8)
            terms[pl.ds(first, channels), :] = product[i * channels : (i + 1) * channels]
    count = local_res * pieces
    outer = jnp.concatenate(
        [terms[pl.ds(c, count, stride=pitch), :].astype(jnp.bfloat16) for c in range(channels)], axis=1
    )
    owner = lax.broadcasted_iota(jnp.int32, outer.shape, 1) % lanes // channels
    spread = jnp.concatenate(
        [jnp.where(owner == j, outer, jnp.zeros_like(outer)) for j in range(per_piece)], axis=0
    )
    weight = jnp.concatenate(
        [weight_ref[c * channels : (c + 1) * channels] for c in range(channels) for _ in range(per_piece)], axis=0
    )
    total = jnp.dot(spread, weight, preferred_element_type=jnp.float32)
    total = total * inv_count + bias_ref[...]
    for j in range(per_piece):
        rows[pl.ds(j, count, stride=per_piece), :] = total[j * count : (j + 1) * count]
    out_ref[...] = rows[...].reshape(out_ref.shape).astype(out_ref.dtype)


def on_device(alignment, ln_gain, proj_left, proj_right, out_weight, out_bias):
    seq_shards = lax.axis_size("seq")
    res_shards = lax.axis_size("res")
    local_seqs, local_res, width = alignment.shape
    channels = proj_left.shape[1]
    lanes = local_res * channels
    features = out_weight.shape[1]
    both = pl.pallas_call(
        project_kernel,
        out_shape=jax.ShapeDtypeStruct((2, local_seqs, lanes), jnp.bfloat16),
        in_specs=[VMEM] * 4,
        out_specs=VMEM,
    )(alignment.reshape(local_seqs, local_res * width), ln_gain.reshape(1, width), proj_left.T, proj_right.T)

    pieces = res_shards // seq_shards
    res = lax.axis_index("res")
    seq = lax.axis_index("seq")
    axes = ("res", "seq")

    def swap(value, bits, cross):
        pairs = [
            (r * seq_shards + q, (r ^ bits) * seq_shards + (q ^ cross))
            for r in range(res_shards)
            for q in range(seq_shards)
        ]
        return lax.ppermute(value, axes, pairs)

    other = lax.ppermute(both, "seq", [(0, 1), (1, 0)])
    first = seq == 0
    full = jnp.concatenate((jnp.where(first, both, other), jnp.where(first, other, both)), axis=1)
    left, right = full[0], full[1]
    far = swap(right, pieces, 1)
    home = res // pieces == seq
    mine = jnp.where(home, right, far)
    yours = jnp.where(home, far, right)
    rights = [mine] + [None] * (pieces - 1)
    for n in sorted(range(1, pieces), key=lambda n: -bin(n).count("1")):
        rights[n] = swap(yours, n, 1)

    place = (res % pieces).reshape(1)
    pitch = channels + 8
    return pl.pallas_call(
        functools.partial(pair_kernel, pitch),
        out_shape=jax.ShapeDtypeStruct((local_res, pieces * local_res, features), jnp.bfloat16),
        in_specs=[pl.BlockSpec(memory_space=pltpu.SMEM)] + [VMEM] * (pieces + 3),
        out_specs=VMEM,
        scratch_shapes=[
            pltpu.VMEM((local_res * pieces * pitch, lanes), jnp.float32),
            pltpu.VMEM((local_res * pieces * local_res, features), jnp.float32),
        ],
    )(place, left, *rights, out_weight, out_bias.reshape(1, features))


def swaps_fit(mesh):
    res_shards, seq_shards = mesh.shape["res"], mesh.shape["seq"]
    return seq_shards == 2 and res_shards in (2, 4, 8)


def solution(mesh):
    placed = (P(("groups", "seq"), "res", None), P(), P(), P(), P(), P())
    return jax.shard_map(
        on_device if swaps_fit(mesh) else gathered,
        mesh=mesh,
        in_specs=placed,
        out_specs=P(("groups", "res"), "seq", None),
        check_vma=False,
    )
```

```python
import functools
import math

import jax
import jax.numpy as jnp
from jax import lax
from jax.experimental import pallas as pl
from jax.experimental.pallas import tpu as pltpu
from jax.sharding import PartitionSpec as P

def normalize(alignment, ln_gain):
    values = alignment.astype(jnp.float32)
    centred = values - jnp.mean(values, axis=-1, keepdims=True)
    variance = jnp.mean(centred * centred, axis=-1, keepdims=True)
    return (centred * lax.rsqrt(variance + 1e-05) * ln_gain).astype(jnp.bfloat16)


def pair_block(left_flat, columns, weight_full, inv_count):
    channels = columns.shape[2]
    col_count = columns.shape[1]
    row_count = left_flat.shape[1] // channels
    block_width = math.gcd(col_count, 64)

    def advance(position, totals):
        column_block = lax.dynamic_slice_in_dim(columns, position * block_width, block_width, 1)
        right_flat = column_block.reshape(columns.shape[0], block_width * channels)
        outer_terms = (
            lax.dot_general(
                left_flat, right_flat, (((0,), (0,)), ((), ())), preferred_element_type=jnp.float32
            )
            * inv_count
        )
        outer_terms = outer_terms.reshape(row_count, channels, block_width, channels).transpose(
            0, 2, 1, 3
        )
        outer_terms = outer_terms.reshape(row_count * block_width, channels * channels)
        projected = jnp.dot(outer_terms, weight_full, precision=lax.Precision.HIGHEST)
        projected = projected.reshape(row_count, block_width, weight_full.shape[1])
        return lax.dynamic_update_slice_in_dim(totals, projected, position * block_width, 1)

    totals = jnp.zeros((row_count, col_count, weight_full.shape[1]), jnp.float32)
    return lax.fori_loop(0, col_count // block_width, advance, totals)


def gathered(alignment, ln_gain, proj_left, proj_right, out_weight, out_bias):
    seq_shards = lax.axis_size("seq")
    local_seqs = alignment.shape[0]
    local_res = alignment.shape[1]
    channels = proj_left.shape[1]
    inv_count = 1.0 / (local_seqs * seq_shards)
    normed = normalize(alignment, ln_gain)
    flat_rows = normed.reshape(-1, normed.shape[2])
    both_sides = jnp.dot(
        flat_rows, jnp.concatenate((proj_left, proj_right), 1), preferred_element_type=jnp.float32
    )
    both_sides = both_sides.astype(jnp.bfloat16).reshape(local_seqs, local_res, 2 * channels)
    left_side = both_sides[:, :, :channels]
    right_side = both_sides[:, :, channels:]
    weight_full = out_weight.astype(jnp.float32)
    left_all = lax.all_gather(left_side, "seq", axis=0, tiled=True)
    left_flat = left_all.reshape(left_all.shape[0], local_res * channels)
    right_all = lax.all_gather(right_side, "res", axis=1, tiled=True)
    split_right = right_all.reshape(
        local_seqs, seq_shards, right_all.shape[1] // seq_shards, channels
    )
    arrived = lax.all_to_all(split_right, "seq", split_axis=1, concat_axis=0, tiled=True)
    squeezed = arrived.reshape(arrived.shape[0], arrived.shape[2], arrived.shape[3])
    summed = pair_block(left_flat, squeezed, weight_full, inv_count)
    return (summed + out_bias).astype(jnp.bfloat16)


VMEM = pl.BlockSpec(memory_space=pltpu.VMEM)
HBM = pl.BlockSpec(memory_space=pltpu.HBM)


def near(value):
    return pltpu.with_memory_space_constraint(value, pltpu.VMEM)


def project_kernel(x_hbm, gain_hbm, left_hbm, right_hbm, both_ref, x_ref, gain_ref, left_ref, right_ref, rows, sems):
    copies = [
        pltpu.make_async_copy(source, target, sems.at[n])
        for n, (source, target) in enumerate(
            ((x_hbm, x_ref), (gain_hbm, gain_ref), (left_hbm, left_ref), (right_hbm, right_ref))
        )
    ]
    for copy in copies:
        copy.start()
    for copy in copies:
        copy.wait()
    seqs, local_res, width = x_ref.shape
    tiles, _, lanes = rows.shape
    for n in range(tiles):
        part = x_ref[:, :, n * lanes : (n + 1) * lanes].astype(jnp.float32)
        rows[n] = part.reshape(seqs * local_res, lanes)
    sides = ([], [])
    for r in range(local_res):
        values = jnp.concatenate(
            [rows[n, pl.ds(r, seqs, stride=local_res), :] for n in range(tiles)], axis=1
        )
        centred = values - jnp.mean(values, axis=-1, keepdims=True)
        variance = jnp.mean(centred * centred, axis=-1, keepdims=True)
        normed = (centred * lax.rsqrt(variance + 1e-05) * gain_ref[...]).astype(jnp.bfloat16)
        for side, weight_ref in zip(sides, (left_ref, right_ref)):
            side.append(
                lax.dot_general(
                    normed, weight_ref[...], (((1,), (1,)), ((), ())),
                    preferred_element_type=jnp.float32,
                )
            )
    for n, side in enumerate(sides):
        both_ref[n] = jnp.concatenate(side, axis=1).astype(jnp.bfloat16)


def pair_kernel(pitch, place_ref, left_ref, *refs):
    *right_refs, weight_ref, bias_hbm, out_ref, terms, rows, bias_ref, sem = refs
    bias_copy = pltpu.make_async_copy(bias_hbm, bias_ref, sem)
    bias_copy.start()
    pieces = len(right_refs)
    local_res, _, features = out_ref.shape
    lanes = left_ref.shape[1]
    channels = lanes // local_res
    per_piece = lanes // channels
    inv_count = 1.0 / left_ref.shape[0]
    left_t = left_ref[...].T
    for n, right_ref in enumerate(right_refs):
        product = jnp.dot(left_t, right_ref[...], preferred_element_type=jnp.float32)
        at = place_ref[0] ^ n
        for i in range(local_res):
            first = pl.multiple_of((i * pieces + at) * pitch, 8)
            terms[pl.ds(first, channels), :] = product[i * channels : (i + 1) * channels]
    count = local_res * pieces
    outer = jnp.concatenate(
        [terms[pl.ds(c, count, stride=pitch), :].astype(jnp.bfloat16) for c in range(channels)], axis=1
    )
    owner = lax.broadcasted_iota(jnp.int32, outer.shape, 1) % lanes // channels
    spread = jnp.concatenate(
        [jnp.where(owner == j, outer, jnp.zeros_like(outer)) for j in range(per_piece)], axis=0
    )
    weight = jnp.concatenate(
        [weight_ref[c * channels : (c + 1) * channels] for c in range(channels) for _ in range(per_piece)], axis=0
    )
    total = jnp.dot(spread, weight, preferred_element_type=jnp.float32)
    bias_copy.wait()
    total = total * inv_count + bias_ref[...]
    for j in range(per_piece):
        rows[pl.ds(j, count, stride=per_piece), :] = total[j * count : (j + 1) * count]
    out_ref[...] = rows[...].reshape(out_ref.shape).astype(out_ref.dtype)


def on_device(alignment, ln_gain, proj_left, proj_right, out_weight, out_bias):
    seq_shards = lax.axis_size("seq")
    res_shards = lax.axis_size("res")
    local_seqs, local_res, width = alignment.shape
    channels = proj_left.shape[1]
    lanes = local_res * channels
    features = out_weight.shape[1]
    both = pl.pallas_call(
        project_kernel,
        out_shape=pltpu.VMEM((2, local_seqs, lanes), jnp.bfloat16),
        in_specs=[HBM] * 4,
        out_specs=VMEM,
        scratch_shapes=[
            pltpu.VMEM(alignment.shape, alignment.dtype),
            pltpu.VMEM((1, width), jnp.float32),
            pltpu.VMEM((channels, width), proj_left.dtype),
            pltpu.VMEM((channels, width), proj_right.dtype),
            pltpu.VMEM((width // 128, local_seqs * local_res, 128), jnp.float32),
            pltpu.SemaphoreType.DMA((4,)),
        ],
    )(alignment, ln_gain.reshape(1, width), proj_left.T, proj_right.T)

    pieces = res_shards // seq_shards
    res = lax.axis_index("res")
    seq = lax.axis_index("seq")
    axes = ("res", "seq")

    def swap(value, bits, cross):
        pairs = [
            (r * seq_shards + q, (r ^ bits) * seq_shards + (q ^ cross))
            for r in range(res_shards)
            for q in range(seq_shards)
        ]
        return lax.ppermute(value, axes, pairs)

    other = lax.ppermute(both, "seq", [(0, 1), (1, 0)])
    first = seq == 0
    full = jnp.concatenate((jnp.where(first, both, other), jnp.where(first, other, both)), axis=1)
    left, right = full[0], full[1]
    far = swap(right, pieces, 1)
    home = res // pieces == seq
    mine = jnp.where(home, right, far)
    yours = jnp.where(home, far, right)
    rights = [mine] + [None] * (pieces - 1)
    for n in sorted(range(1, pieces), key=lambda n: -bin(n).count("1")):
        rights[n] = swap(yours, n, 1)

    place = (res % pieces).reshape(1)
    pitch = channels + 8
    return pl.pallas_call(
        functools.partial(pair_kernel, pitch),
        out_shape=jax.ShapeDtypeStruct((local_res, pieces * local_res, features), jnp.bfloat16),
        in_specs=[pl.BlockSpec(memory_space=pltpu.SMEM)] + [VMEM] * (pieces + 2) + [HBM],
        out_specs=VMEM,
        scratch_shapes=[
            pltpu.VMEM((local_res * pieces * pitch, lanes), jnp.float32),
            pltpu.VMEM((local_res * pieces * local_res, features), jnp.float32),
            pltpu.VMEM((1, features), jnp.float32),
            pltpu.SemaphoreType.DMA(()),
        ],
    )(place, *(near(v) for v in (left, *rights, out_weight)), out_bias.reshape(1, features))


def swaps_fit(mesh):
    res_shards, seq_shards = mesh.shape["res"], mesh.shape["seq"]
    return seq_shards == 2 and res_shards in (2, 4, 8)


def solution(mesh):
    placed = (P(("groups", "seq"), "res", None), P(), P(), P(), P(), P())
    return jax.shard_map(
        on_device if swaps_fit(mesh) else gathered,
        mesh=mesh,
        in_specs=placed,
        out_specs=P(("groups", "res"), "seq", None),
        check_vma=False,
    )
```

```python
import functools
import math

import jax
import jax.numpy as jnp
from jax import lax
from jax.experimental import pallas as pl
from jax.experimental.pallas import tpu as pltpu
from jax.sharding import PartitionSpec as P


def normalize(alignment, ln_gain):
    values = alignment.astype(jnp.float32)
    centred = values - jnp.mean(values, axis=-1, keepdims=True)
    variance = jnp.mean(centred * centred, axis=-1, keepdims=True)
    return (centred * lax.rsqrt(variance + 1e-05) * ln_gain).astype(jnp.bfloat16)


def pair_block(left_flat, columns, weight_full, inv_count):
    channels = columns.shape[2]
    col_count = columns.shape[1]
    row_count = left_flat.shape[1] // channels
    block_width = math.gcd(col_count, 64)

    def advance(position, totals):
        column_block = lax.dynamic_slice_in_dim(columns, position * block_width, block_width, 1)
        right_flat = column_block.reshape(columns.shape[0], block_width * channels)
        outer_terms = (
            lax.dot_general(
                left_flat, right_flat, (((0,), (0,)), ((), ())), preferred_element_type=jnp.float32
            )
            * inv_count
        )
        outer_terms = outer_terms.reshape(row_count, channels, block_width, channels).transpose(
            0, 2, 1, 3
        )
        outer_terms = outer_terms.reshape(row_count * block_width, channels * channels)
        projected = jnp.dot(outer_terms, weight_full, precision=lax.Precision.HIGHEST)
        projected = projected.reshape(row_count, block_width, weight_full.shape[1])
        return lax.dynamic_update_slice_in_dim(totals, projected, position * block_width, 1)

    totals = jnp.zeros((row_count, col_count, weight_full.shape[1]), jnp.float32)
    return lax.fori_loop(0, col_count // block_width, advance, totals)


def gathered(alignment, ln_gain, proj_left, proj_right, out_weight, out_bias):
    seq_shards = lax.axis_size("seq")
    local_seqs = alignment.shape[0]
    local_res = alignment.shape[1]
    channels = proj_left.shape[1]
    inv_count = 1.0 / (local_seqs * seq_shards)
    normed = normalize(alignment, ln_gain)
    flat_rows = normed.reshape(-1, normed.shape[2])
    both_sides = jnp.dot(
        flat_rows, jnp.concatenate((proj_left, proj_right), 1), preferred_element_type=jnp.float32
    )
    both_sides = both_sides.astype(jnp.bfloat16).reshape(local_seqs, local_res, 2 * channels)
    left_side = both_sides[:, :, :channels]
    right_side = both_sides[:, :, channels:]
    weight_full = out_weight.astype(jnp.float32)
    left_all = lax.all_gather(left_side, "seq", axis=0, tiled=True)
    left_flat = left_all.reshape(left_all.shape[0], local_res * channels)
    right_all = lax.all_gather(right_side, "res", axis=1, tiled=True)
    split_right = right_all.reshape(
        local_seqs, seq_shards, right_all.shape[1] // seq_shards, channels
    )
    arrived = lax.all_to_all(split_right, "seq", split_axis=1, concat_axis=0, tiled=True)
    squeezed = arrived.reshape(arrived.shape[0], arrived.shape[2], arrived.shape[3])
    summed = pair_block(left_flat, squeezed, weight_full, inv_count)
    return (summed + out_bias).astype(jnp.bfloat16)


VMEM = pl.BlockSpec(memory_space=pltpu.VMEM)
HBM = pl.BlockSpec(memory_space=pltpu.HBM)


def near(value):
    return pltpu.with_memory_space_constraint(value, pltpu.VMEM)


def project_kernel(x_hbm, gain_hbm, left_hbm, right_hbm, both_ref, x_ref, gain_ref, left_ref, right_ref, rows, sems):
    copies = [
        pltpu.make_async_copy(source, target, sems.at[n])
        for n, (source, target) in enumerate(
            ((x_hbm, x_ref), (gain_hbm, gain_ref), (left_hbm, left_ref), (right_hbm, right_ref))
        )
    ]
    for copy in copies:
        copy.start()
    copies[0].wait()
    seqs, local_res, _ = x_ref.shape
    tiles, _, lanes = rows.shape
    for n in range(tiles):
        part = x_ref[:, :, n * lanes : (n + 1) * lanes].astype(jnp.float32)
        rows[n] = part.reshape(seqs * local_res, lanes)
    for copy in copies[1:]:
        copy.wait()
    sides = ([], [])
    for r in range(local_res):
        values = jnp.concatenate(
            [rows[n, pl.ds(r, seqs, stride=local_res), :] for n in range(tiles)], axis=1
        )
        centred = values - jnp.mean(values, axis=-1, keepdims=True)
        variance = jnp.mean(centred * centred, axis=-1, keepdims=True)
        normed = (centred * lax.rsqrt(variance + 1e-05) * gain_ref[...]).astype(jnp.bfloat16)
        for side, weight_ref in zip(sides, (left_ref, right_ref)):
            side.append(
                lax.dot_general(
                    normed, weight_ref[...], (((1,), (1,)), ((), ())),
                    preferred_element_type=jnp.float32,
                )
            )
    for n, side in enumerate(sides):
        both_ref[n] = jnp.concatenate(side, axis=1).astype(jnp.bfloat16)


def pair_rows(left_t, pieces, places, local_res, weight_ref, terms, totals, rows):
    count = local_res * len(pieces)
    channels = left_t.shape[0] // local_res
    lanes = pieces[0].shape[1]
    per_piece = lanes // channels
    pitch = terms.shape[0] // count
    for n, piece in enumerate(pieces):
        product = jnp.dot(left_t, piece, preferred_element_type=jnp.float32)
        for i in range(local_res):
            first = (i * len(pieces) + n) * pitch
            terms[first : first + channels, :] = product[i * channels : (i + 1) * channels]
    owner = lax.broadcasted_iota(jnp.int32, (count, lanes), 1) // channels
    spread = []
    for c in range(channels):
        term = terms[pl.ds(c, count, stride=pitch), :]
        parts = [jnp.where(owner == j, term, 0.0) for j in range(per_piece)]
        spread.append(jnp.concatenate(parts, axis=0).astype(jnp.bfloat16))
    weight = jnp.concatenate(
        [weight_ref[c * channels : (c + 1) * channels] for c in range(channels) for _ in range(per_piece)], axis=0
    )
    totals[...] = jnp.dot(jnp.concatenate(spread, axis=1), weight, preferred_element_type=jnp.float32)
    columns = rows.shape[0] // local_res
    for n, at in enumerate(places):
        for j in range(per_piece):
            row = totals[pl.ds(j * count + n, local_res, stride=len(pieces)), :]
            rows[pl.ds(at * per_piece + j, local_res, stride=columns), :] = row


def early_kernel(
    local_res, slots, place_ref, left_ref, right_ref, weight_ref, bias_hbm, left_t_ref, rows, bias_ref, terms, totals, sem
):
    bias_copy = pltpu.make_async_copy(bias_hbm, bias_ref, sem)
    bias_copy.start()
    left_t_ref[...] = left_ref[...].T
    seqs = left_ref.shape[0]
    pieces = [right_ref[n * seqs : (n + 1) * seqs] for n in range(len(slots))]
    places = [place_ref[0] ^ slot for slot in slots]
    rows[...] = jnp.zeros_like(rows)
    pair_rows(left_t_ref[...], pieces, places, local_res, weight_ref, terms, totals, rows)
    bias_copy.wait()


def late_kernel(
    slots, place_ref, left_t_ref, early_ref, right_ref, weight_ref, bias_ref, out_ref, rows, terms, totals
):
    rows[...] = early_ref[...]
    seqs = left_t_ref.shape[1]
    pieces = [right_ref[n * seqs : (n + 1) * seqs] for n in range(len(slots))]
    places = [place_ref[0] ^ slot for slot in slots]
    pair_rows(left_t_ref[...], pieces, places, out_ref.shape[0], weight_ref, terms, totals, rows)
    total = rows[...] * (1.0 / seqs) + bias_ref[...]
    out_ref[...] = total.reshape(out_ref.shape).astype(out_ref.dtype)


def on_device(alignment, ln_gain, proj_left, proj_right, out_weight, out_bias):
    seq_shards = lax.axis_size("seq")
    res_shards = lax.axis_size("res")
    local_seqs, local_res, width = alignment.shape
    channels = proj_left.shape[1]
    lanes = local_res * channels
    features = out_weight.shape[1]
    both = pl.pallas_call(
        project_kernel,
        out_shape=pltpu.VMEM((2, local_seqs, lanes), jnp.bfloat16),
        in_specs=[HBM] * 4,
        out_specs=VMEM,
        scratch_shapes=[
            pltpu.VMEM(alignment.shape, alignment.dtype),
            pltpu.VMEM((1, width), jnp.float32),
            pltpu.VMEM((channels, width), proj_left.dtype),
            pltpu.VMEM((channels, width), proj_right.dtype),
            pltpu.VMEM((width // 128, local_seqs * local_res, 128), jnp.float32),
            pltpu.SemaphoreType.DMA((4,)),
        ],
    )(alignment, ln_gain.reshape(1, width), proj_left.T, proj_right.T)

    pieces = res_shards // seq_shards
    res = lax.axis_index("res")
    seq = lax.axis_index("seq")
    half = res_shards // 2

    def send(value, target):
        pairs = []
        for r in range(res_shards):
            for q in range(seq_shards):
                to_res, to_seq = target(r, q)
                pairs.append((r * seq_shards + q, to_res * seq_shards + to_seq))
        return lax.ppermute(value, ("res", "seq"), pairs)

    def flow(far, near_by):
        def target(r, q):
            if q == 0:
                return r ^ half ^ far, int(r >= half)
            return (r ^ 1, 1) if r >= half else (r ^ near_by, 0)

        return target

    other = lax.ppermute(both, "seq", [(0, 1), (1, 0)])
    first = seq == 0
    full = jnp.concatenate((jnp.where(first, both, other), jnp.where(first, other, both)), axis=1)
    left, right = full[0], full[1]
    home = res // half == seq
    one = send(right, flow(0, 1))
    two = send(right, flow(1, 0))
    mine = jnp.concatenate((jnp.where(home, right, one), jnp.where(home, one, two)), 0)
    late = send(mine, lambda r, q: (r ^ 2, q))
    slots = (0, 1, 2, 3)
    nseq = right.shape[0]
    place = (res % half).reshape(1)
    weight = near(out_weight)
    columns = pieces * local_res
    pitch = channels + 8
    count = local_res * 2
    smem = pl.BlockSpec(memory_space=pltpu.SMEM)
    scratch = [
        pltpu.VMEM((count * pitch, lanes), jnp.float32),
        pltpu.VMEM((count * local_res, features), jnp.float32),
    ]
    left_t, early, bias = pl.pallas_call(
        functools.partial(early_kernel, local_res, slots[:2]),
        out_shape=[
            pltpu.VMEM((lanes, nseq), jnp.bfloat16),
            pltpu.VMEM((local_res * columns, features), jnp.float32),
            pltpu.VMEM((1, features), jnp.float32),
        ],
        in_specs=[smem] + [VMEM] * 3 + [HBM],
        out_specs=[VMEM] * 3,
        scratch_shapes=scratch + [pltpu.SemaphoreType.DMA(())],
        cost_estimate=pl.CostEstimate(flops=10**9, transcendentals=0, bytes_accessed=0),
        name="early",
    )(place, near(left), near(mine), weight, out_bias.reshape(1, features))
    return pl.pallas_call(
        functools.partial(late_kernel, slots[2:]),
        out_shape=jax.ShapeDtypeStruct((local_res, columns, features), jnp.bfloat16),
        in_specs=[smem] + [VMEM] * 5,
        out_specs=VMEM,
        scratch_shapes=[pltpu.VMEM((local_res * columns, features), jnp.float32)] + scratch,
        name="late",
    )(place, near(left_t), near(early), near(late), weight, near(bias))


def swaps_fit(mesh):
    return mesh.shape["seq"] == 2 and mesh.shape["res"] == 8


def solution(mesh):
    placed = (P(("groups", "seq"), "res", None), P(), P(), P(), P(), P())
    return jax.shard_map(
        on_device if swaps_fit(mesh) else gathered,
        mesh=mesh,
        in_specs=placed,
        out_specs=P(("groups", "res"), "seq", None),
        check_vma=False,
    )
```

```python
import functools
import math

import jax
import jax.numpy as jnp
from jax import lax
from jax.experimental import pallas as pl
from jax.experimental.pallas import tpu as pltpu
from jax.sharding import PartitionSpec as P


def normalize(alignment, ln_gain):
    values = alignment.astype(jnp.float32)
    centred = values - jnp.mean(values, axis=-1, keepdims=True)
    variance = jnp.mean(centred * centred, axis=-1, keepdims=True)
    return (centred * lax.rsqrt(variance + 1e-05) * ln_gain).astype(jnp.bfloat16)


def pair_block(left_flat, columns, weight_full, inv_count):
    channels = columns.shape[2]
    col_count = columns.shape[1]
    row_count = left_flat.shape[1] // channels
    block_width = math.gcd(col_count, 64)

    def advance(position, totals):
        column_block = lax.dynamic_slice_in_dim(columns, position * block_width, block_width, 1)
        right_flat = column_block.reshape(columns.shape[0], block_width * channels)
        outer_terms = (
            lax.dot_general(
                left_flat, right_flat, (((0,), (0,)), ((), ())), preferred_element_type=jnp.float32
            )
            * inv_count
        )
        outer_terms = outer_terms.reshape(row_count, channels, block_width, channels).transpose(
            0, 2, 1, 3
        )
        outer_terms = outer_terms.reshape(row_count * block_width, channels * channels)
        projected = jnp.dot(outer_terms, weight_full, precision=lax.Precision.HIGHEST)
        projected = projected.reshape(row_count, block_width, weight_full.shape[1])
        return lax.dynamic_update_slice_in_dim(totals, projected, position * block_width, 1)

    totals = jnp.zeros((row_count, col_count, weight_full.shape[1]), jnp.float32)
    return lax.fori_loop(0, col_count // block_width, advance, totals)


def gathered(alignment, ln_gain, proj_left, proj_right, out_weight, out_bias):
    seq_shards = lax.axis_size("seq")
    local_seqs = alignment.shape[0]
    local_res = alignment.shape[1]
    channels = proj_left.shape[1]
    inv_count = 1.0 / (local_seqs * seq_shards)
    normed = normalize(alignment, ln_gain)
    flat_rows = normed.reshape(-1, normed.shape[2])
    both_sides = jnp.dot(
        flat_rows, jnp.concatenate((proj_left, proj_right), 1), preferred_element_type=jnp.float32
    )
    both_sides = both_sides.astype(jnp.bfloat16).reshape(local_seqs, local_res, 2 * channels)
    left_side = both_sides[:, :, :channels]
    right_side = both_sides[:, :, channels:]
    weight_full = out_weight.astype(jnp.float32)
    left_all = lax.all_gather(left_side, "seq", axis=0, tiled=True)
    left_flat = left_all.reshape(left_all.shape[0], local_res * channels)
    right_all = lax.all_gather(right_side, "res", axis=1, tiled=True)
    split_right = right_all.reshape(
        local_seqs, seq_shards, right_all.shape[1] // seq_shards, channels
    )
    arrived = lax.all_to_all(split_right, "seq", split_axis=1, concat_axis=0, tiled=True)
    squeezed = arrived.reshape(arrived.shape[0], arrived.shape[2], arrived.shape[3])
    summed = pair_block(left_flat, squeezed, weight_full, inv_count)
    return (summed + out_bias).astype(jnp.bfloat16)


VMEM = pl.BlockSpec(memory_space=pltpu.VMEM)
HBM = pl.BlockSpec(memory_space=pltpu.HBM)


def near(value):
    return pltpu.with_memory_space_constraint(value, pltpu.VMEM)


def project_kernel(x_hbm, gain_hbm, left_hbm, right_hbm, both_ref, x_ref, gain_ref, left_ref, right_ref, rows, sems):
    copies = [
        pltpu.make_async_copy(source, target, sems.at[n])
        for n, (source, target) in enumerate(
            ((x_hbm, x_ref), (gain_hbm, gain_ref), (left_hbm, left_ref), (right_hbm, right_ref))
        )
    ]
    for copy in copies:
        copy.start()
    copies[0].wait()
    seqs, local_res, _ = x_ref.shape
    tiles, _, lanes = rows.shape
    for n in range(tiles):
        part = x_ref[:, :, n * lanes : (n + 1) * lanes].astype(jnp.float32)
        rows[n] = part.reshape(seqs * local_res, lanes)
    for copy in copies[1:]:
        copy.wait()
    sides = ([], [])
    for r in range(local_res):
        values = jnp.concatenate(
            [rows[n, pl.ds(r, seqs, stride=local_res), :] for n in range(tiles)], axis=1
        )
        centred = values - jnp.mean(values, axis=-1, keepdims=True)
        variance = jnp.mean(centred * centred, axis=-1, keepdims=True)
        normed = (centred * lax.rsqrt(variance + 1e-05) * gain_ref[...]).astype(jnp.bfloat16)
        for side, weight_ref in zip(sides, (left_ref, right_ref)):
            side.append(
                lax.dot_general(
                    normed, weight_ref[...], (((1,), (1,)), ((), ())),
                    preferred_element_type=jnp.float32,
                )
            )
    for n, side in enumerate(sides):
        both_ref[n] = jnp.concatenate(side, axis=1).astype(jnp.bfloat16)


def pair_rows(left_t_ref, pairs, places, local_res, weight_ref, terms, totals, rows):
    left_t = left_t_ref[...]
    lanes, seqs = left_t.shape
    count = local_res * len(places)
    channels = lanes // local_res
    per_piece = lanes // channels
    pitch = channels + 8
    pieces = [ref[first : first + seqs] for ref in pairs for first in range(0, ref.shape[0], seqs)]
    for n, piece in enumerate(pieces):
        product = jnp.dot(left_t, piece, preferred_element_type=jnp.float32)
        for i in range(local_res):
            first = (i * len(pieces) + n) * pitch
            terms[first : first + channels, :] = product[i * channels : (i + 1) * channels]
    owner = lax.broadcasted_iota(jnp.int32, (count, lanes), 1) // channels
    spread = []
    for c in range(channels):
        term = terms[pl.ds(c, count, stride=pitch), :]
        parts = [jnp.where(owner == j, term, 0.0) for j in range(per_piece)]
        spread.append(jnp.concatenate(parts, axis=0).astype(jnp.bfloat16))
    weight = jnp.concatenate(
        [weight_ref[c * channels : (c + 1) * channels] for c in range(channels) for _ in range(per_piece)], axis=0
    )
    totals[: count * per_piece, :] = jnp.dot(
        jnp.concatenate(spread, axis=1), weight, preferred_element_type=jnp.float32
    )
    columns = rows.shape[0] // local_res
    for n, at in enumerate(places):
        for j in range(per_piece):
            row = totals[pl.ds(j * count + n, local_res, stride=len(pieces)), :]
            rows[pl.ds(at * per_piece + j, local_res, stride=columns), :] = row


def early_kernel(
    local_res, step, home_ref, low_ref, from_ref, left_ref, own_ref, one_ref, weight_ref, bias_hbm, left_t_ref, rows, bias_ref, terms, totals, sem
):
    bias_copy = pltpu.make_async_copy(bias_hbm, bias_ref, sem)
    bias_copy.start()
    left_t_ref[...] = left_ref[...].T
    rows[...] = jnp.zeros_like(rows)
    home, low, arrived = home_ref[0], low_ref[0], from_ref[0]

    @pl.when(home == 1)
    def _():
        places = [low, low ^ step, arrived, arrived ^ step]
        pair_rows(left_t_ref, (own_ref, one_ref), places, local_res, weight_ref, terms, totals, rows)

    @pl.when(home == 0)
    def _():
        pair_rows(left_t_ref, (one_ref,), [arrived, arrived ^ step], local_res, weight_ref, terms, totals, rows)

    bias_copy.wait()


def late_kernel(step, home_ref, from_ref, left_t_ref, early_ref, two_ref, weight_ref, bias_ref, out_ref, rows, terms, totals):
    rows[...] = early_ref[...]

    @pl.when(home_ref[0] == 0)
    def _():
        arrived = from_ref[0]
        pair_rows(left_t_ref, (two_ref,), [arrived, arrived ^ step], out_ref.shape[0], weight_ref, terms, totals, rows)

    total = rows[...] * (1.0 / left_t_ref.shape[1]) + bias_ref[...]
    out_ref[...] = total.reshape(out_ref.shape).astype(out_ref.dtype)


def on_device(alignment, ln_gain, proj_left, proj_right, out_weight, out_bias):
    seq_shards = lax.axis_size("seq")
    res_shards = lax.axis_size("res")
    local_seqs, local_res, width = alignment.shape
    channels = proj_left.shape[1]
    lanes = local_res * channels
    features = out_weight.shape[1]
    both = pl.pallas_call(
        project_kernel,
        out_shape=pltpu.VMEM((2, local_seqs, lanes), jnp.bfloat16),
        in_specs=[HBM] * 4,
        out_specs=VMEM,
        scratch_shapes=[
            pltpu.VMEM(alignment.shape, alignment.dtype),
            pltpu.VMEM((1, width), jnp.float32),
            pltpu.VMEM((channels, width), proj_left.dtype),
            pltpu.VMEM((channels, width), proj_right.dtype),
            pltpu.VMEM((width // 128, local_seqs * local_res, 128), jnp.float32),
            pltpu.SemaphoreType.DMA((4,)),
        ],
    )(alignment, ln_gain.reshape(1, width), proj_left.T, proj_right.T)

    pieces = res_shards // seq_shards
    res = lax.axis_index("res")
    seq = lax.axis_index("seq")
    half = res_shards // 2

    def send(value, target):
        pairs = []
        for r in range(res_shards):
            for q in range(seq_shards):
                to_res, to_seq = target(r, q)
                pairs.append((r * seq_shards + q, to_res * seq_shards + to_seq))
        return lax.ppermute(value, ("res", "seq"), pairs)

    other = lax.ppermute(both, "seq", [(0, 1), (1, 0)])
    first = seq == 0
    full = jnp.concatenate((jnp.where(first, both, other), jnp.where(first, other, both)), axis=1)
    left, right = full[0], full[1]
    home = res // half == seq

    def flow(served, offsets):
        def target(r, q):
            k = r // half * 2 + q
            return served[k] // 2 * half + (r % half ^ offsets[k]), served[k] % 2

        return target

    cross = flow((1, 0, 3, 2), (1, 1, 1, 1))
    round_one = flow((2, 0, 3, 1), (0, 2, 2, 2))
    round_two = flow((2, 0, 3, 1), (2, 0, 0, 0))
    pair = jnp.concatenate((right, send(right, cross)), 0)
    one = send(pair, round_one)
    two = send(pair, round_two)
    low = res % half
    served_from_lower = jnp.logical_and(res >= half, seq == 0)
    from_one_value = low ^ jnp.where(served_from_lower, 0, 2)
    from_two_value = low ^ jnp.where(served_from_lower, 2, 0)
    at_home = home.astype(jnp.int32).reshape(1)
    from_one = from_one_value.reshape(1)
    from_two = from_two_value.reshape(1)
    nseq = right.shape[0]
    weight = near(out_weight)
    columns = pieces * local_res
    pitch = channels + 8
    count = local_res * pieces
    smem = pl.BlockSpec(memory_space=pltpu.SMEM)
    scratch = [
        pltpu.VMEM((count * pitch, lanes), jnp.float32),
        pltpu.VMEM((count * local_res, features), jnp.float32),
    ]
    left_t, early, bias = pl.pallas_call(
        functools.partial(early_kernel, local_res, 1),
        out_shape=[
            pltpu.VMEM((lanes, nseq), jnp.bfloat16),
            pltpu.VMEM((local_res * columns, features), jnp.float32),
            pltpu.VMEM((1, features), jnp.float32),
        ],
        in_specs=[smem] * 3 + [VMEM] * 4 + [HBM],
        out_specs=[VMEM] * 3,
        scratch_shapes=scratch + [pltpu.SemaphoreType.DMA(())],
        cost_estimate=pl.CostEstimate(flops=10**9, transcendentals=0, bytes_accessed=0),
        name="early",
    )(at_home, low.reshape(1), from_one, near(left), near(pair), near(one), weight, out_bias.reshape(1, features))
    return pl.pallas_call(
        functools.partial(late_kernel, 1),
        out_shape=jax.ShapeDtypeStruct((local_res, columns, features), jnp.bfloat16),
        in_specs=[smem] * 2 + [VMEM] * 5,
        out_specs=VMEM,
        scratch_shapes=[pltpu.VMEM((local_res * columns, features), jnp.float32)] + scratch,
        name="late",
    )(at_home, from_two, near(left_t), near(early), near(two), weight, near(bias))


def swaps_fit(mesh):
    return mesh.shape["seq"] == 2 and mesh.shape["res"] == 8


def solution(mesh):
    placed = (P(("groups", "seq"), "res", None), P(), P(), P(), P(), P())
    return jax.shard_map(
        on_device if swaps_fit(mesh) else gathered,
        mesh=mesh,
        in_specs=placed,
        out_specs=P(("groups", "res"), "seq", None),
        check_vma=False,
    )
```

```python
import functools
import math

import jax
import jax.numpy as jnp
from jax import lax
from jax.experimental import pallas as pl
from jax.experimental.pallas import tpu as pltpu
from jax.sharding import PartitionSpec as P


def normalize(alignment, ln_gain):
    values = alignment.astype(jnp.float32)
    centred = values - jnp.mean(values, axis=-1, keepdims=True)
    variance = jnp.mean(centred * centred, axis=-1, keepdims=True)
    return (centred * lax.rsqrt(variance + 1e-05) * ln_gain).astype(jnp.bfloat16)


def pair_block(left_flat, columns, weight_full, inv_count):
    channels = columns.shape[2]
    col_count = columns.shape[1]
    row_count = left_flat.shape[1] // channels
    block_width = math.gcd(col_count, 64)

    def advance(position, totals):
        column_block = lax.dynamic_slice_in_dim(columns, position * block_width, block_width, 1)
        right_flat = column_block.reshape(columns.shape[0], block_width * channels)
        outer_terms = (
            lax.dot_general(
                left_flat, right_flat, (((0,), (0,)), ((), ())), preferred_element_type=jnp.float32
            )
            * inv_count
        )
        outer_terms = outer_terms.reshape(row_count, channels, block_width, channels).transpose(
            0, 2, 1, 3
        )
        outer_terms = outer_terms.reshape(row_count * block_width, channels * channels)
        projected = jnp.dot(outer_terms, weight_full, precision=lax.Precision.HIGHEST)
        projected = projected.reshape(row_count, block_width, weight_full.shape[1])
        return lax.dynamic_update_slice_in_dim(totals, projected, position * block_width, 1)

    totals = jnp.zeros((row_count, col_count, weight_full.shape[1]), jnp.float32)
    return lax.fori_loop(0, col_count // block_width, advance, totals)


def gathered(alignment, ln_gain, proj_left, proj_right, out_weight, out_bias):
    seq_shards = lax.axis_size("seq")
    local_seqs = alignment.shape[0]
    local_res = alignment.shape[1]
    channels = proj_left.shape[1]
    inv_count = 1.0 / (local_seqs * seq_shards)
    normed = normalize(alignment, ln_gain)
    flat_rows = normed.reshape(-1, normed.shape[2])
    both_sides = jnp.dot(
        flat_rows, jnp.concatenate((proj_left, proj_right), 1), preferred_element_type=jnp.float32
    )
    both_sides = both_sides.astype(jnp.bfloat16).reshape(local_seqs, local_res, 2 * channels)
    left_side = both_sides[:, :, :channels]
    right_side = both_sides[:, :, channels:]
    weight_full = out_weight.astype(jnp.float32)
    left_all = lax.all_gather(left_side, "seq", axis=0, tiled=True)
    left_flat = left_all.reshape(left_all.shape[0], local_res * channels)
    right_all = lax.all_gather(right_side, "res", axis=1, tiled=True)
    split_right = right_all.reshape(
        local_seqs, seq_shards, right_all.shape[1] // seq_shards, channels
    )
    arrived = lax.all_to_all(split_right, "seq", split_axis=1, concat_axis=0, tiled=True)
    squeezed = arrived.reshape(arrived.shape[0], arrived.shape[2], arrived.shape[3])
    summed = pair_block(left_flat, squeezed, weight_full, inv_count)
    return (summed + out_bias).astype(jnp.bfloat16)


VMEM = pl.BlockSpec(memory_space=pltpu.VMEM)
HBM = pl.BlockSpec(memory_space=pltpu.HBM)


def near(value):
    return pltpu.with_memory_space_constraint(value, pltpu.VMEM)


def project_kernel(
    x_hbm, gain_hbm, left_hbm, right_hbm, bias_hbm, both_ref, bias_ref, x_ref, gain_ref, left_ref, right_ref, rows, sems
):
    copies = [
        pltpu.make_async_copy(source, target, sems.at[n])
        for n, (source, target) in enumerate(
            (
                (x_hbm, x_ref), (gain_hbm, gain_ref), (left_hbm, left_ref), (right_hbm, right_ref), (bias_hbm, bias_ref)
            )
        )
    ]
    for copy in copies:
        copy.start()
    copies[0].wait()
    seqs, local_res, _ = x_ref.shape
    tiles, _, lanes = rows.shape
    for n in range(tiles):
        part = x_ref[:, :, n * lanes : (n + 1) * lanes].astype(jnp.float32)
        rows[n] = part.reshape(seqs * local_res, lanes)
    for copy in copies[1:-1]:
        copy.wait()
    sides = ([], [])
    for r in range(local_res):
        values = jnp.concatenate(
            [rows[n, pl.ds(r, seqs, stride=local_res), :] for n in range(tiles)], axis=1
        )
        centred = values - jnp.mean(values, axis=-1, keepdims=True)
        variance = jnp.mean(centred * centred, axis=-1, keepdims=True)
        normed = (centred * lax.rsqrt(variance + 1e-05) * gain_ref[...]).astype(jnp.bfloat16)
        for side, weight_ref in zip(sides, (left_ref, right_ref)):
            side.append(
                lax.dot_general(
                    normed, weight_ref[...], (((1,), (1,)), ((), ())),
                    preferred_element_type=jnp.float32,
                )
            )
    for n, side in enumerate(sides):
        both_ref[n] = jnp.concatenate(side, axis=1).astype(jnp.bfloat16)
    copies[-1].wait()


def pair_rows(left_t_ref, pairs, places, local_res, weight_ref, terms, totals, rows):
    left_t = left_t_ref[...]
    lanes, seqs = left_t.shape
    count = local_res * len(places)
    channels = lanes // local_res
    per_piece = lanes // channels
    pitch = channels + 8
    pieces = [ref[first : first + seqs] for ref in pairs for first in range(0, ref.shape[0], seqs)]
    for n, piece in enumerate(pieces):
        product = jnp.dot(left_t, piece, preferred_element_type=jnp.float32)
        for i in range(local_res):
            first = (i * len(pieces) + n) * pitch
            terms[first : first + channels, :] = product[i * channels : (i + 1) * channels]
    owner = lax.broadcasted_iota(jnp.int32, (count, lanes), 1) // channels
    spread = []
    for c in range(channels):
        term = terms[pl.ds(c, count, stride=pitch), :]
        parts = [jnp.where(owner == j, term, 0.0) for j in range(per_piece)]
        spread.append(jnp.concatenate(parts, axis=0).astype(jnp.bfloat16))
    weight = jnp.concatenate(
        [weight_ref[c * channels : (c + 1) * channels] for c in range(channels) for _ in range(per_piece)], axis=0
    )
    totals[: count * per_piece, :] = jnp.dot(
        jnp.concatenate(spread, axis=1), weight, preferred_element_type=jnp.float32
    )
    columns = rows.shape[0] // local_res
    for n, at in enumerate(places):
        for j in range(per_piece):
            row = totals[pl.ds(j * count + n, local_res, stride=len(pieces)), :]
            rows[pl.ds(at * per_piece + j, local_res, stride=columns), :] = row


def turn_kernel(left_ref, left_t_ref):
    left_t_ref[...] = left_ref[...].T


def write_out(rows, inv_count, bias_ref, out_hbm, packed, sem):
    total = rows[...] * inv_count + bias_ref[...]
    packed[...] = total.reshape(packed.shape).astype(packed.dtype)
    copy = pltpu.make_async_copy(packed, out_hbm, sem)
    copy.start()
    copy.wait()


def early_kernel(
    step, home_ref, low_ref, one_at_ref, left_t_ref, own_ref, one_ref, weight_ref, bias_ref,
    out_hbm, rows, terms, totals, packed, sem
):
    low, one_at = low_ref[0], one_at_ref[0]
    local_res = packed.shape[0]

    @pl.when(home_ref[0] == 1)
    def _():
        places = [low, low ^ step, one_at, one_at ^ step]
        pair_rows(left_t_ref, (own_ref, one_ref), places, local_res, weight_ref, terms, totals, rows)
        write_out(rows, 1.0 / left_t_ref.shape[1], bias_ref, out_hbm, packed, sem)

    @pl.when(home_ref[0] == 0)
    def _():
        rows[...] = jnp.zeros_like(rows)
        pair_rows(left_t_ref, (one_ref,), [one_at, one_at ^ step], local_res, weight_ref, terms, totals, rows)


def late_kernel(
    step, home_ref, two_at_ref, left_t_ref, two_ref, weight_ref, bias_ref, early_rows, early_hbm,
    out_hbm, rows, terms, totals, packed, sem
):
    two_at = two_at_ref[0]

    @pl.when(home_ref[0] == 0)
    def _():
        rows[...] = early_rows[...]
        pair_rows(left_t_ref, (two_ref,), [two_at, two_at ^ step], packed.shape[0], weight_ref, terms, totals, rows)
        write_out(rows, 1.0 / left_t_ref.shape[1], bias_ref, out_hbm, packed, sem)


def on_device(alignment, ln_gain, proj_left, proj_right, out_weight, out_bias):
    seq_shards = lax.axis_size("seq")
    res_shards = lax.axis_size("res")
    local_seqs, local_res, width = alignment.shape
    channels = proj_left.shape[1]
    lanes = local_res * channels
    features = out_weight.shape[1]
    both, bias = pl.pallas_call(
        project_kernel,
        out_shape=[
            pltpu.VMEM((2, local_seqs, lanes), jnp.bfloat16),
            pltpu.VMEM((1, features), jnp.float32),
        ],
        in_specs=[HBM] * 5,
        out_specs=[VMEM] * 2,
        scratch_shapes=[
            pltpu.VMEM(alignment.shape, alignment.dtype),
            pltpu.VMEM((1, width), jnp.float32),
            pltpu.VMEM((channels, width), proj_left.dtype),
            pltpu.VMEM((channels, width), proj_right.dtype),
            pltpu.VMEM((width // 128, local_seqs * local_res, 128), jnp.float32),
            pltpu.SemaphoreType.DMA((5,)),
        ],
        name="project",
    )(alignment, ln_gain.reshape(1, width), proj_left.T, proj_right.T, out_bias.reshape(1, features))

    pieces = res_shards // seq_shards
    res = lax.axis_index("res")
    seq = lax.axis_index("seq")
    half = res_shards // 2

    def send(value, target):
        pairs = []
        for r in range(res_shards):
            for q in range(seq_shards):
                to_res, to_seq = target(r, q)
                pairs.append((r * seq_shards + q, to_res * seq_shards + to_seq))
        return lax.ppermute(value, ("res", "seq"), pairs)

    other = lax.ppermute(both, "seq", [(0, 1), (1, 0)])
    first = seq == 0
    full = jnp.concatenate((jnp.where(first, both, other), jnp.where(first, other, both)), axis=1)
    left, right = full[0], full[1]
    home = res // half == seq

    def flow(served, offsets):
        def target(r, q):
            k = r // half * 2 + q
            return served[k] // 2 * half + (r % half ^ offsets[k]), served[k] % 2

        return target

    cross = flow((1, 0, 3, 2), (1, 1, 1, 1))
    round_one = flow((2, 0, 3, 1), (0, 2, 2, 2))
    round_two = flow((2, 0, 3, 1), (2, 0, 0, 0))
    pair = jnp.concatenate((right, send(right, cross)), 0)
    one = send(pair, round_one)
    two = send(pair, round_two)
    low = res % half
    served_from_lower = jnp.logical_and(res >= half, seq == 0)
    from_one_value = low ^ jnp.where(served_from_lower, 0, 2)
    from_two_value = low ^ jnp.where(served_from_lower, 2, 0)
    at_home = home.astype(jnp.int32).reshape(1)
    one_at = from_one_value.reshape(1)
    two_at = from_two_value.reshape(1)
    weight = near(out_weight)
    bias = near(bias)
    columns = pieces * local_res
    count = local_res * pieces
    smem = pl.BlockSpec(memory_space=pltpu.SMEM)
    out = jax.ShapeDtypeStruct((local_res, columns, features), jnp.bfloat16)
    rows = pltpu.VMEM((local_res * columns, features), jnp.float32)
    scratch = [
        pltpu.VMEM((count * (channels + 8), lanes), jnp.float32),
        pltpu.VMEM((count * local_res, features), jnp.float32),
        pltpu.VMEM(out.shape, out.dtype),
        pltpu.SemaphoreType.DMA(()),
    ]
    left_t = near(
        pl.pallas_call(
            turn_kernel,
            out_shape=pltpu.VMEM((lanes, left.shape[0]), jnp.bfloat16),
            in_specs=[VMEM],
            out_specs=VMEM,
            name="turn",
        )(near(left))
    )
    early, early_rows = pl.pallas_call(
        functools.partial(early_kernel, 1),
        out_shape=[out, rows],
        in_specs=[smem] * 3 + [VMEM] * 5,
        out_specs=[HBM, VMEM],
        scratch_shapes=scratch,
        cost_estimate=pl.CostEstimate(flops=10**9, transcendentals=0, bytes_accessed=0),
        name="early",
    )(at_home, low.reshape(1), one_at, left_t, near(pair), near(one), weight, bias)
    return pl.pallas_call(
        functools.partial(late_kernel, 1),
        out_shape=out,
        in_specs=[smem] * 2 + [VMEM] * 5 + [HBM],
        out_specs=HBM,
        scratch_shapes=[rows] + scratch,
        input_output_aliases={7: 0},
        name="late",
    )(at_home, two_at, left_t, near(two), weight, bias, near(early_rows), early)


def swaps_fit(mesh):
    return mesh.shape["seq"] == 2 and mesh.shape["res"] == 8


def solution(mesh):
    placed = (P(("groups", "seq"), "res", None), P(), P(), P(), P(), P())
    return jax.shard_map(
        on_device if swaps_fit(mesh) else gathered,
        mesh=mesh,
        in_specs=placed,
        out_specs=P(("groups", "res"), "seq", None),
        check_vma=False,
    )
```
